32 devices in a mesh: expert: 8 (over z, y), tensor: 4 (over x, core).
Axes of the slice: x: 2, y: 2, z: 4, core: 2. Of those that a mesh axis runs over, the one named last changes fastest.
Arguments:
- tokens: bfloat16 [1024, 2048], P('expert', 'tensor'), may hold values from -6 to 6
- grad_out: bfloat16 [1024, 2048], P('expert', 'tensor'), may hold values from -6 to 6
- route_weights: float32 [1024, 8], P('expert'), may hold values from 0.02 to 0.5
- expert_ids: int32 [1024, 8], P('expert'), may hold values from 0 to 15, all different within a row; in each aligned block of 128 rows (0 to 127, 128 to 255, ...) at most 96 rows name the same one
- gate_weight: bfloat16 [16, 2048, 768], P('expert', None, 'tensor'), may hold values from -0.125 to 0.125
- up_weight: bfloat16 [16, 2048, 768], P('expert', None, 'tensor'), may hold values from -0.125 to 0.125
- down_weight: bfloat16 [16, 768, 2048], P('expert', 'tensor'), may hold values from -0.21875 to 0.21875
- gate_adapter_first: bfloat16 [16, 2048, 64], P('expert'), may hold values from -0.125 to 0.125
- gate_adapter_second: bfloat16 [16, 64, 768], P('expert', None, 'tensor'), may hold values from -0.75 to 0.75
- up_adapter_first: bfloat16 [16, 2048, 64], P('expert'), may hold values from -0.125 to 0.125
- up_adapter_second: bfloat16 [16, 64, 768], P('expert', None, 'tensor'), may hold values from -0.75 to 0.75
- down_adapter_first: bfloat16 [16, 768, 64], P('expert', 'tensor'), may hold values from -0.21875 to 0.21875
- down_adapter_second: bfloat16 [16, 64, 2048], P('expert'), may hold values from -0.75 to 0.75
Outputs:
- grad_tokens: bfloat16 [1024, 2048], P('expert', 'tensor')
- gate_first_gradient: float32 [16, 2048, 64], P('expert', 'tensor')
- gate_second_gradient: float32 [16, 64, 768], P('expert', None, 'tensor')
- up_first_gradient: float32 [16, 2048, 64], P('expert', 'tensor')
- up_second_gradient: float32 [16, 64, 768], P('expert', None, 'tensor')
- down_first_gradient: float32 [16, 768, 64], P('expert', 'tensor')
- down_second_gradient: float32 [16, 64, 2048], P('expert', None, 'tensor')
The draws below stay inside these ranges and needn't reach their ends.
Inputs may be any that keep to these rules, and one draw needn't show every extreme that they name: `expert_ids`: each token names 8 different experts. Among the 128 rows of one device no expert is named more than 96 times, a bound that some block reaches.
All inputs are finite; a program needn't handle non-finite values.
Results may differ from the reference program's by a relative error of at most 0.012.
Values may be sent and summed in bfloat16 or wider, within the bound.
A program may use at most 128 MiB of HBM per device.

```python
import math
import jax
import jax.numpy as jnp
import numpy as np
from jax import lax

D = 2048
FF = 768
TOP = 8
R = 64
TOK_DEV = 128
EXPERTS = 16
CAP = 96
TOKENS = 1024
N_EXPERT = 8
N_TENSOR = 4


def block_scale(key, extent, pieces, least, high):
    factor_of = 1.0
    for dim, blocks in pieces:
        draws = jax.random.uniform(jax.random.fold_in(jax.random.fold_in(key, 6), dim), (blocks,), jnp.float32, least / len(pieces), high / len(pieces))
        factor_of = factor_of * jnp.repeat(jnp.exp(draws), extent[dim] // blocks).reshape((-1,) + (1,) * (len(extent) - 1 - dim))
    return factor_of


def deal_out(rng, own, number, rows, number_of, top, limit, lean):
    sequence = jax.random.permutation(rng, number_of)
    crowded, common = load_shares(number_of, rows * top, limit, lean, True), load_shares(number_of, rows * top, limit, lean, False)
    places = jnp.arange(number_of)

    def named(lengths, rotation):
        used = int((lengths > 0).sum())
        fixed = max(1, used // 4)
        passed = fixed + (places - fixed + rotation * (used - fixed)) % max(1, number_of - fixed)
        return jnp.zeros((number_of,), jnp.int32).at[sequence[jnp.where(places < fixed, places, passed)]].set(jnp.asarray(lengths, jnp.int32))

    lengths = jnp.where(number % 4 == 0, named(crowded, number // 4), named(common, number - number // 4 - 1))
    mixed = jax.random.permutation(jax.random.fold_in(own, 3), number_of)
    donor, sink = mixed[0:number_of // 2 * 2:2], mixed[1:number_of // 2 * 2:2]
    slack = jnp.minimum(lengths[donor] - 1, limit - lengths[sink]) // 2
    slack = jnp.where((donor == sequence[0]) | (sink == sequence[0]) | (lengths[sink] == 0), 0, jnp.maximum(slack, 0))
    passed = jax.random.randint(jax.random.fold_in(own, 4), (number_of // 2,), 0, 1 << 20) % (slack + 1)
    lengths = lengths.at[donor].add(-passed).at[sink].add(passed)
    items = jnp.searchsorted(jnp.cumsum(lengths), jnp.arange(rows * top), side="right").astype(jnp.int32)
    table = items.reshape(top, rows).T
    table = table[jax.random.permutation(jax.random.fold_in(own, 1), rows)]
    rotation = jax.random.randint(jax.random.fold_in(own, 2), (rows, 1), 0, top)
    return jnp.take_along_axis(table, (jnp.arange(top)[None, :] + rotation) % top, axis=1)


def load_shares(number_of, total, limit, skew, full):
    portions = [(1 << 20) // math.isqrt(standing ** skew) + 1 for standing in range(1, number_of + 1)]
    largest = limit if full else min(limit, max(-(-total // number_of), total * portions[0] // sum(portions)))
    least = 1 if total - largest >= number_of - 1 else 0
    given, spare = [largest] + [least] * (number_of - 1), total - largest - least * (number_of - 1)
    while spare > 0:
        free = [i for i in range(1, number_of) if given[i] < largest] or [i for i in range(1, number_of) if given[i] < limit]
        whole, budget = sum([portions[i] for i in free]), spare
        for i in free:
            more = min(limit - given[i], max(1, budget * portions[i] // whole), spare)
            given[i] = given[i] + more
            spare = spare - more
    return np.array(given)


def bell_draw(rng, dims, deviation, reach, shards=(), kind=jnp.bfloat16):
    drawn = jax.random.normal(rng, dims, jnp.float32) * deviation
    if len(shards) > 0:
        drawn = block_scale(rng, dims, shards, -0.22, 0.18) * drawn
    return jnp.clip(drawn, min=-reach, max=reach).astype(kind)


def setup_inputs(seed: int = 0) -> dict:
    key_list = jax.random.split(jax.random.key(seed), 14)
    tokens = bell_draw(key_list[0], (TOKENS, D), 1.0, 6.0, ((0, 8), (1, 4)))
    grad_out = bell_draw(key_list[1], (TOKENS, D), 1.0, 6.0, ((0, 8), (1, 4)))
    route_weights = jnp.clip(jnp.exp(math.log(0.5) - 3.218876 * jax.random.uniform(key_list[2], (TOKENS, TOP), jnp.float32) ** block_scale(key_list[2], (TOKENS, TOP), ((0, 8),), -0.2, 0.2)), 0.02, 0.5)
    expert_ids_keys = jax.random.split(jax.random.fold_in(key_list[3], 1), TOKENS // TOK_DEV)
    expert_ids_turns = jax.random.permutation(jax.random.fold_in(key_list[3], 3), TOKENS // TOK_DEV)
    expert_ids = jax.vmap(lambda own, number: deal_out(jax.random.fold_in(key_list[3], 2), own, number, TOK_DEV, EXPERTS, TOP, CAP, 2))(expert_ids_keys, expert_ids_turns).reshape((TOKENS, TOP))
    gate_weight = bell_draw(key_list[4], (EXPERTS, D, FF), D ** -0.5, 0.125, ((0, 8), (2, 4)))
    up_weight = bell_draw(key_list[5], (EXPERTS, D, FF), D ** -0.5, 0.125, ((0, 8), (2, 4)))
    down_weight = bell_draw(key_list[6], (EXPERTS, FF, D), FF ** -0.5, 0.21875, ((0, 8), (1, 4)))
    gate_adapter_first = bell_draw(key_list[7], (EXPERTS, D, R), D ** -0.5, 0.125, ((0, 8),))
    gate_adapter_second = bell_draw(key_list[8], (EXPERTS, R, FF), R ** -0.5, 0.75, ((0, 8), (2, 4)))
    up_adapter_first = bell_draw(key_list[9], (EXPERTS, D, R), D ** -0.5, 0.125, ((0, 8),))
    up_adapter_second = bell_draw(key_list[10], (EXPERTS, R, FF), R ** -0.5, 0.75, ((0, 8), (2, 4)))
    down_adapter_first = bell_draw(key_list[11], (EXPERTS, FF, R), FF ** -0.5, 0.21875, ((0, 8), (1, 4)))
    down_adapter_second = bell_draw(key_list[12], (EXPERTS, R, D), R ** -0.5, 0.75, ((0, 8),))
    return dict(tokens=tokens, grad_out=grad_out, route_weights=route_weights, expert_ids=expert_ids, gate_weight=gate_weight, up_weight=up_weight, down_weight=down_weight, gate_adapter_first=gate_adapter_first, gate_adapter_second=gate_adapter_second, up_adapter_first=up_adapter_first, up_adapter_second=up_adapter_second, down_adapter_first=down_adapter_first, down_adapter_second=down_adapter_second)


adapter_scale = 0.5


def expert_pass(routed_input, routed_gradient, gate_weight, up_weight, down_weight, gate_adapter_first, gate_adapter_second, up_adapter_first, up_adapter_second, down_adapter_first, down_adapter_second):
    single_float = jnp.float32
    brain_float_half = jnp.bfloat16
    adapter_gate_term = jnp.dot(routed_input, gate_adapter_first, preferred_element_type=single_float).astype(brain_float_half)
    adapter_up_term = jnp.dot(routed_input, up_adapter_first, preferred_element_type=single_float).astype(brain_float_half)
    gate_activation = jnp.dot(routed_input, gate_weight, preferred_element_type=single_float) + adapter_scale * jnp.dot(adapter_gate_term, gate_adapter_second, preferred_element_type=single_float)
    up_activation = jnp.dot(routed_input, up_weight, preferred_element_type=single_float) + adapter_scale * jnp.dot(adapter_up_term, up_adapter_second, preferred_element_type=single_float)
    sigma = jax.nn.sigmoid(gate_activation)
    active = gate_activation * sigma
    hidden_activation = (active * up_activation).astype(brain_float_half)
    down_adapter_term = jnp.dot(hidden_activation, down_adapter_first, preferred_element_type=single_float).astype(brain_float_half)
    backward_adapter_term = jnp.dot(routed_gradient, down_adapter_second.T, preferred_element_type=single_float).astype(brain_float_half)
    hidden_gradient = jnp.dot(routed_gradient, down_weight.T, preferred_element_type=single_float) + adapter_scale * jnp.dot(backward_adapter_term, down_adapter_first.T, preferred_element_type=single_float)
    gate_gradient = (hidden_gradient * up_activation * sigma * (1.0 + gate_activation * (1.0 - sigma))).astype(brain_float_half)
    up_gradient = (hidden_gradient * active).astype(brain_float_half)
    gate_backward = jnp.dot(gate_gradient, gate_adapter_second.T, preferred_element_type=single_float).astype(brain_float_half)
    up_backward = jnp.dot(up_gradient, up_adapter_second.T, preferred_element_type=single_float).astype(brain_float_half)
    grads = (
        adapter_scale * jnp.dot(routed_input.T, gate_backward, preferred_element_type=single_float),
        adapter_scale * jnp.dot(adapter_gate_term.T, gate_gradient, preferred_element_type=single_float),
        adapter_scale * jnp.dot(routed_input.T, up_backward, preferred_element_type=single_float),
        adapter_scale * jnp.dot(adapter_up_term.T, up_gradient, preferred_element_type=single_float),
        adapter_scale * jnp.dot(hidden_activation.T, backward_adapter_term, preferred_element_type=single_float),
        adapter_scale * jnp.dot(down_adapter_term.T, routed_gradient, preferred_element_type=single_float),
    )
    block_width = FF // N_TENSOR
    total = jnp.zeros((routed_input.shape[0], D), single_float)
    for block in range(N_TENSOR):
        lower = block * block_width
        upper = lower + block_width
        gate_portion = jnp.dot(gate_gradient[:, lower:upper], gate_adapter_second[:, lower:upper].T, preferred_element_type=single_float).astype(brain_float_half)
        up_portion = jnp.dot(up_gradient[:, lower:upper], up_adapter_second[:, lower:upper].T, preferred_element_type=single_float).astype(brain_float_half)
        merged_result = jnp.dot(gate_gradient[:, lower:upper], gate_weight[:, lower:upper].T, preferred_element_type=single_float)
        merged_result = merged_result + jnp.dot(up_gradient[:, lower:upper], up_weight[:, lower:upper].T, preferred_element_type=single_float)
        merged_result = merged_result + adapter_scale * (jnp.dot(gate_portion, gate_adapter_first.T, preferred_element_type=single_float) + jnp.dot(up_portion, up_adapter_first.T, preferred_element_type=single_float))
        total = total + merged_result.astype(brain_float_half).astype(single_float)
    return grads, total


def reference(tokens, grad_out, route_weights, expert_ids, gate_weight, up_weight, down_weight, gate_adapter_first, gate_adapter_second, up_adapter_first, up_adapter_second, down_adapter_first, down_adapter_second):
    single_float = jnp.float32
    brain_float_half = jnp.bfloat16
    blocks = expert_ids.reshape(N_EXPERT, TOK_DEV, TOP)
    numbers = jnp.arange(EXPERTS, dtype=jnp.int32)
    picked = jnp.any(blocks[:, :, :, None] == numbers[None, None, None, :], axis=2).astype(jnp.int32)
    before = jnp.cumsum(picked, axis=1) - picked
    slot_index = jnp.take_along_axis(before, blocks, axis=2).astype(jnp.int32)
    source = jnp.broadcast_to(jnp.arange(N_EXPERT, dtype=jnp.int32)[:, None, None], blocks.shape)
    assigned = jnp.arange(TOKENS * TOP, dtype=jnp.int32).reshape(blocks.shape)
    sentinel = TOKENS * TOP
    table = jnp.full((N_EXPERT, EXPERTS, CAP), sentinel, jnp.int32).at[source, blocks, slot_index].set(assigned)
    per_expert = jnp.transpose(table, (1, 0, 2)).reshape(EXPERTS, N_EXPERT * CAP)
    flat_weights = route_weights.reshape(-1)

    def step(accum, items):
        index, wg, wu, wd, ag, bg, au, bu, ad, bd = items
        live = index < sentinel
        safe = jnp.minimum(index, sentinel - 1)
        token_row = (safe // TOP).astype(jnp.int32)
        routed_input = jnp.where(live[:, None], tokens[token_row].astype(single_float), 0.0).astype(brain_float_half)
        factor = jnp.where(live, flat_weights[safe], 0.0)
        routed_gradient = (factor[:, None] * grad_out[token_row].astype(single_float)).astype(brain_float_half)
        grads, total = expert_pass(routed_input, routed_gradient, wg, wu, wd, ag, bg, au, bu, ad, bd)
        accum = accum.at[token_row].add(jnp.where(live[:, None], total, 0.0))
        return accum, grads

    accum, grads = lax.scan(step, jnp.zeros((TOKENS, D), single_float), (per_expert, gate_weight, up_weight, down_weight, gate_adapter_first, gate_adapter_second, up_adapter_first, up_adapter_second, down_adapter_first, down_adapter_second))
    return (accum.astype(brain_float_half), grads[0], grads[1], grads[2], grads[3], grads[4], grads[5])
```

```python
import jax
import jax.numpy as jnp
from jax import lax
from jax.sharding import PartitionSpec as P

adapter_scale = 0.5


def slot_positions(expert_ids, experts_all, capacity):
    tok_rows = expert_ids.shape[0]
    numbers = lax.broadcasted_iota(jnp.int32, (1, 1, experts_all), 2)
    picked = jnp.sum((expert_ids[:, :, None] == numbers).astype(jnp.float32), axis=1).astype(
        jnp.bfloat16
    )
    row_index = lax.broadcasted_iota(jnp.int32, (tok_rows, tok_rows), 0)
    col_index = lax.broadcasted_iota(jnp.int32, (tok_rows, tok_rows), 1)
    earlier = (row_index > col_index).astype(jnp.bfloat16)
    before = jnp.dot(earlier, picked, preferred_element_type=jnp.float32)
    slot_index = jnp.take_along_axis(before, expert_ids, axis=1).astype(jnp.int32)
    return expert_ids * capacity + slot_index


def fill_slots(values, positions, slot_count):
    width = values.shape[-1]
    flat = values.reshape(-1, width)
    return jnp.zeros((slot_count, width), values.dtype).at[positions.reshape(-1)].set(flat)


def routed_plan(
    tokens,
    grad_out,
    route_weights,
    expert_ids,
    gate_weight,
    up_weight,
    down_weight,
    gate_adapter_first,
    gate_adapter_second,
    up_adapter_first,
    up_adapter_second,
    down_adapter_first,
    down_adapter_second,
):
    single_float = jnp.float32
    brain_float_half = jnp.bfloat16
    tok_rows, top_count = expert_ids.shape
    local_experts = gate_weight.shape[0]
    sources = lax.axis_size("expert")
    experts_all = local_experts * sources
    capacity = 3 * tok_rows * top_count // (2 * experts_all)
    slot_count = experts_all * capacity
    positions = slot_positions(expert_ids, experts_all, capacity)
    width = tokens.shape[1]
    spread_in = jnp.broadcast_to(tokens[:, None, :], (tok_rows, top_count, width))
    scaled = (route_weights[:, :, None] * grad_out[:, None, :].astype(single_float)).astype(
        brain_float_half
    )
    send_in = fill_slots(spread_in, positions, slot_count)
    send_grad = fill_slots(scaled, positions, slot_count)
    part_in, part_grad = (
        lax.all_to_all(send_in, "expert", split_axis=0, concat_axis=0, tiled=True),
        lax.all_to_all(send_grad, "expert", split_axis=0, concat_axis=0, tiled=True),
    )
    recv_in, recv_grad = (
        lax.all_gather(part_in, "tensor", axis=1, tiled=True),
        lax.all_gather(part_grad, "tensor", axis=1, tiled=True),
    )
    hidden_width = recv_in.shape[1]
    routed_input = recv_in.reshape(sources, local_experts, capacity, hidden_width)
    routed_gradient = recv_grad.reshape(sources, local_experts, capacity, hidden_width)
    slice_width = hidden_width // lax.axis_size("tensor")
    slice_start = lax.axis_index("tensor") * slice_width
    adapter_gate_term = jnp.einsum(
        "mbtk,bkz->mbtz", routed_input, gate_adapter_first, preferred_element_type=single_float
    ).astype(brain_float_half)
    adapter_up_term = jnp.einsum(
        "mbtk,bkz->mbtz", routed_input, up_adapter_first, preferred_element_type=single_float
    ).astype(brain_float_half)
    gate_activation = jnp.einsum(
        "secd,edf->secf", routed_input, gate_weight, preferred_element_type=single_float
    )
    gate_activation = gate_activation + adapter_scale * jnp.einsum(
        "imal,mlt->imat",
        adapter_gate_term,
        gate_adapter_second,
        preferred_element_type=single_float,
    )
    up_activation = jnp.einsum(
        "secd,edf->secf", routed_input, up_weight, preferred_element_type=single_float
    )
    up_activation = up_activation + adapter_scale * jnp.einsum(
        "imal,mlt->imat", adapter_up_term, up_adapter_second, preferred_element_type=single_float
    )
    sigma = jax.nn.sigmoid(gate_activation)
    active = gate_activation * sigma
    hidden_activation = (active * up_activation).astype(brain_float_half)
    down_part = jnp.einsum(
        "secf,efr->secr", hidden_activation, down_adapter_first, preferred_element_type=single_float
    )
    down_total = lax.psum(down_part.astype(jnp.bfloat16), "tensor").astype(jnp.float32)
    backward_adapter_term = jnp.einsum(
        "secd,erd->secr", routed_gradient, down_adapter_second, preferred_element_type=single_float
    ).astype(brain_float_half)
    hidden_gradient = jnp.einsum(
        "secd,efd->secf", routed_gradient, down_weight, preferred_element_type=single_float
    )
    hidden_gradient = hidden_gradient + adapter_scale * jnp.einsum(
        "oamh,ath->oamt",
        backward_adapter_term,
        down_adapter_first,
        preferred_element_type=single_float,
    )
    gate_gradient = (
        hidden_gradient * up_activation * sigma * (1.0 + gate_activation * (1.0 - sigma))
    ).astype(brain_float_half)
    upward_gradient = (hidden_gradient * active).astype(brain_float_half)
    gate_part = jnp.einsum(
        "secf,erf->secr", gate_gradient, gate_adapter_second, preferred_element_type=single_float
    )
    up_part = jnp.einsum(
        "secf,erf->secr", upward_gradient, up_adapter_second, preferred_element_type=single_float
    )
    joined_weight = jnp.concatenate(
        (gate_weight, up_weight, gate_adapter_first, up_adapter_first), axis=2
    )
    joined_grad = jnp.concatenate(
        (
            gate_gradient,
            upward_gradient,
            gate_part.astype(brain_float_half) * adapter_scale,
            up_part.astype(brain_float_half) * adapter_scale,
        ),
        axis=3,
    )
    input_portion = (
        jnp.einsum(
            "secf,edf->secd", joined_grad, joined_weight, preferred_element_type=single_float
        )
        .astype(brain_float_half)
        .reshape(slot_count, hidden_width)
    )
    gate_total, up_total = (
        lax.psum(gate_part.astype(jnp.bfloat16), "tensor").astype(jnp.float32),
        lax.psum(up_part.astype(jnp.bfloat16), "tensor").astype(jnp.float32),
    )
    in_slice = lax.dynamic_slice_in_dim(routed_input, slice_start, slice_width, 3)
    grad_slice = lax.dynamic_slice_in_dim(routed_gradient, slice_start, slice_width, 3)
    gate_first_gradient = adapter_scale * jnp.einsum(
        "secd,secr->edr",
        in_slice,
        gate_total.astype(brain_float_half),
        preferred_element_type=single_float,
    )
    up_first_gradient = adapter_scale * jnp.einsum(
        "secd,secr->edr",
        in_slice,
        up_total.astype(brain_float_half),
        preferred_element_type=single_float,
    )
    gate_second_gradient = adapter_scale * jnp.einsum(
        "zdbq,zdbx->dqx", adapter_gate_term, gate_gradient, preferred_element_type=single_float
    )
    up_second_gradient = adapter_scale * jnp.einsum(
        "zdbq,zdbx->dqx", adapter_up_term, upward_gradient, preferred_element_type=single_float
    )
    down_first_gradient = adapter_scale * jnp.einsum(
        "qoax,qoap->oxp",
        hidden_activation,
        backward_adapter_term,
        preferred_element_type=single_float,
    )
    down_second_gradient = adapter_scale * jnp.einsum(
        "secr,secd->erd",
        down_total.astype(brain_float_half),
        grad_slice,
        preferred_element_type=single_float,
    )
    reduced = lax.psum_scatter(
        input_portion.astype(single_float).astype(jnp.bfloat16),
        "tensor",
        scatter_dimension=1,
        tiled=True,
    ).astype(jnp.float32)
    returned = lax.all_to_all(
        reduced.astype(jnp.bfloat16), "expert", split_axis=0, concat_axis=0, tiled=True
    ).astype(reduced.dtype)
    grad_tokens = jnp.sum(returned[positions], axis=1).astype(brain_float_half)
    return (
        grad_tokens,
        gate_first_gradient,
        gate_second_gradient,
        up_first_gradient,
        up_second_gradient,
        down_first_gradient,
        down_second_gradient,
    )


def block_diagonal(blocks):
    count = len(blocks)
    rows = []
    for i, block in enumerate(blocks):
        rows.append(
            jnp.concatenate(
                [block if i == j else jnp.zeros_like(blocks[j]) for j in range(count)], axis=1
            )
        )
    return jnp.concatenate(rows, axis=0)


def diagonal_blocks(matrix, count):
    height, width = matrix.shape[0] // count, matrix.shape[1] // count
    return jnp.stack(
        [matrix[i * height : (i + 1) * height, i * width : (i + 1) * width] for i in range(count)]
    )


def widen(columns, width):
    rows, count = columns.shape
    return jnp.concatenate(
        [jnp.broadcast_to(columns[:, i : i + 1], (rows, width)) for i in range(count)], axis=1
    )


def dot(a, b):
    return lax.dot_general(a, b, (((1,), (0,)), ((), ())), preferred_element_type=jnp.float32)


def dot_t(a, b):
    return lax.dot_general(a, b, (((1,), (1,)), ((), ())), preferred_element_type=jnp.float32)


def t_dot(a, b):
    return lax.dot_general(a, b, (((0,), (0,)), ((), ())), preferred_element_type=jnp.float32)


def swap_near(value):
    count = lax.axis_size("tensor")
    return lax.ppermute(value, "tensor", [(i, i ^ 1) for i in range(count)])


def swap_far(value):
    count = lax.axis_size("tensor")
    return lax.ppermute(value, "tensor", [(i, (i + count // 2) % count) for i in range(count)])


def pair_order(index, mine, theirs):
    return jnp.where(index == 0, mine, theirs), jnp.where(index == 0, theirs, mine)


def total_over_tensor(part):
    near = part.astype(jnp.bfloat16)
    pair = (near.astype(jnp.float32) + swap_near(near).astype(jnp.float32)).astype(jnp.bfloat16)
    return (pair.astype(jnp.float32) + swap_far(pair).astype(jnp.float32)).astype(jnp.bfloat16)


def dense_plan(
    tokens,
    grad_out,
    route_weights,
    expert_ids,
    gate_weight,
    up_weight,
    down_weight,
    gate_adapter_first,
    gate_adapter_second,
    up_adapter_first,
    up_adapter_second,
    down_adapter_first,
    down_adapter_second,
):
    half = jnp.bfloat16
    single = jnp.float32
    tok_rows, width = tokens.shape
    local_experts, hidden_width, units = gate_weight.shape
    rank = gate_adapter_first.shape[2]
    experts_all = local_experts * lax.axis_size("expert")
    span = local_experts * units
    ranks = local_experts * rank
    place = lax.axis_index("tensor")
    far, near = place // 2, place % 2

    def half_rows(value):
        first, second = pair_order(far, value, swap_far(value))
        joined = jnp.concatenate((first, second), axis=1)
        return lax.all_gather(joined, "expert", axis=0, tiled=True)

    def all_features(mine):
        even, odd = pair_order(near, mine, swap_near(mine))
        return jnp.concatenate(
            (even[:, :width], odd[:, :width], even[:, width:], odd[:, width:]), axis=1
        )

    tokens_half = half_rows(tokens)
    grad_half = half_rows(grad_out)
    numbers = lax.broadcasted_iota(jnp.int32, (1, 1, experts_all), 2)
    chosen = jnp.sum(
        jnp.where(expert_ids[:, :, None] == numbers, route_weights[:, :, None], 0.0), axis=1
    )
    chosen_all = lax.all_gather(chosen, "expert", axis=0, tiled=True)
    factor = lax.dynamic_slice_in_dim(
        chosen_all, lax.axis_index("expert") * local_experts, local_experts, 1
    )
    experts = range(local_experts)
    joined_weight = jnp.concatenate(
        [gate_weight[e] for e in experts]
        + [up_weight[e] for e in experts]
        + [gate_adapter_first[e] for e in experts]
        + [up_adapter_first[e] for e in experts],
        axis=1,
    )
    back_weight = jnp.concatenate(
        [down_weight[e] for e in experts] + [down_adapter_second[e] for e in experts], axis=0
    )
    gate_second = block_diagonal([gate_adapter_second[e] for e in experts])
    up_second = block_diagonal([up_adapter_second[e] for e in experts])
    down_first = block_diagonal([down_adapter_first[e] for e in experts])
    factor_units = widen(factor, units)
    factor_ranks = widen(factor, rank)

    forward = dot(all_features(tokens_half), joined_weight)
    lora_gate = forward[:, 2 * span : 2 * span + ranks].astype(half)
    lora_up = forward[:, 2 * span + ranks :].astype(half)
    gate = forward[:, :span] + adapter_scale * dot(lora_gate, gate_second)
    up = forward[:, span : 2 * span] + adapter_scale * dot(lora_up, up_second)
    sigma = jax.nn.sigmoid(gate)
    active = gate * sigma
    hidden = (active * up).astype(half)
    down_total = total_over_tensor(dot(hidden, down_first))

    backward = dot_t(all_features(grad_half), back_weight)
    back_lora = (factor_ranks * backward[:, span:]).astype(half)
    grad_hidden = factor_units * backward[:, :span] + adapter_scale * dot_t(back_lora, down_first)
    grad_gate = (grad_hidden * up * sigma * (1.0 + gate * (1.0 - sigma))).astype(half)
    grad_up = (grad_hidden * active).astype(half)
    parts = jnp.concatenate((dot_t(grad_gate, gate_second), dot_t(grad_up, up_second)), axis=1)
    parts = parts.astype(half)
    joined_grad = jnp.concatenate((grad_gate, grad_up, parts * adapter_scale), axis=1)
    portion = dot_t(joined_grad, joined_weight).astype(half)
    portion = portion.reshape(portion.shape[0], 2, 2, width)
    keep = lax.dynamic_index_in_dim(portion, near, 2, keepdims=False)
    give = lax.dynamic_index_in_dim(portion, 1 - near, 2, keepdims=False)
    pair = (keep.astype(single) + swap_near(give).astype(single)).astype(half)
    pair = pair.reshape(pair.shape[0], 2 * width)
    summed = lax.psum_scatter(pair, "expert", scatter_dimension=0, tiled=True)
    summed_keep = lax.dynamic_slice_in_dim(summed, far * width, width, 1)
    summed_give = lax.dynamic_slice_in_dim(summed, (1 - far) * width, width, 1)
    grad_tokens = (summed_keep.astype(single) + swap_far(summed_give).astype(single)).astype(half)

    parts_total = total_over_tensor(parts)
    in_slice = lax.dynamic_slice_in_dim(tokens_half, far * width, width, 1)
    grad_slice = lax.dynamic_slice_in_dim(grad_half, far * width, width, 1)
    first = adapter_scale * t_dot(in_slice, parts_total)
    first = first.reshape(width, 2, local_experts, rank).transpose(1, 2, 0, 3)
    weighted = (factor_ranks * down_total.astype(single)).astype(half)
    down_second_gradient = adapter_scale * t_dot(weighted, grad_slice)
    return (
        grad_tokens,
        first[0],
        diagonal_blocks(adapter_scale * t_dot(lora_gate, grad_gate), local_experts),
        first[1],
        diagonal_blocks(adapter_scale * t_dot(lora_up, grad_up), local_experts),
        diagonal_blocks(adapter_scale * t_dot(hidden, back_lora), local_experts),
        down_second_gradient.reshape(local_experts, rank, width),
    )


def local(*arrays):
    tok_rows, top_count = arrays[3].shape
    local_experts = arrays[4].shape[0]
    capacity = 3 * tok_rows * top_count // (2 * local_experts * lax.axis_size("expert"))
    if local_experts * capacity >= tok_rows and lax.axis_size("tensor") == 2 * 2:
        return dense_plan(*arrays)
    return routed_plan(*arrays)


def solution(mesh):
    return jax.shard_map(
        local,
        mesh=mesh,
        in_specs=(
            P("expert", "tensor"),
            P("expert", "tensor"),
            P("expert", None),
            P("expert", None),
            P("expert", None, "tensor"),
            P("expert", None, "tensor"),
            P("expert", "tensor", None),
            P("expert", None, None),
            P("expert", None, "tensor"),
            P("expert", None, None),
            P("expert", None, "tensor"),
            P("expert", "tensor", None),
            P("expert", None, None),
        ),
        out_specs=(
            P("expert", "tensor"),
            P("expert", "tensor", None),
            P("expert", None, "tensor"),
            P("expert", "tensor", None),
            P("expert", None, "tensor"),
            P("expert", "tensor", None),
            P("expert", None, "tensor"),
        ),
        check_vma=False,
    )
```

```python
import functools

import jax
import jax.numpy as jnp
from jax import lax
from jax.experimental import pallas as pl
from jax.experimental.pallas import tpu as pltpu
from jax.sharding import PartitionSpec as P

adapter_scale = 0.5


def slot_positions(expert_ids, experts_all, capacity):
    tok_rows = expert_ids.shape[0]
    numbers = lax.broadcasted_iota(jnp.int32, (1, 1, experts_all), 2)
    picked = jnp.sum((expert_ids[:, :, None] == numbers).astype(jnp.float32), axis=1).astype(
        jnp.bfloat16
    )
    row_index = lax.broadcasted_iota(jnp.int32, (tok_rows, tok_rows), 0)
    col_index = lax.broadcasted_iota(jnp.int32, (tok_rows, tok_rows), 1)
    earlier = (row_index > col_index).astype(jnp.bfloat16)
    before = jnp.dot(earlier, picked, preferred_element_type=jnp.float32)
    slot_index = jnp.take_along_axis(before, expert_ids, axis=1).astype(jnp.int32)
    return expert_ids * capacity + slot_index


def fill_slots(values, positions, slot_count):
    width = values.shape[-1]
    flat = values.reshape(-1, width)
    return jnp.zeros((slot_count, width), values.dtype).at[positions.reshape(-1)].set(flat)


def routed_plan(
    tokens,
    grad_out,
    route_weights,
    expert_ids,
    gate_weight,
    up_weight,
    down_weight,
    gate_adapter_first,
    gate_adapter_second,
    up_adapter_first,
    up_adapter_second,
    down_adapter_first,
    down_adapter_second,
):
    single_float = jnp.float32
    brain_float_half = jnp.bfloat16
    tok_rows, top_count = expert_ids.shape
    local_experts = gate_weight.shape[0]
    sources = lax.axis_size("expert")
    experts_all = local_experts * sources
    capacity = 3 * tok_rows * top_count // (2 * experts_all)
    slot_count = experts_all * capacity
    positions = slot_positions(expert_ids, experts_all, capacity)
    width = tokens.shape[1]
    spread_in = jnp.broadcast_to(tokens[:, None, :], (tok_rows, top_count, width))
    scaled = (route_weights[:, :, None] * grad_out[:, None, :].astype(single_float)).astype(
        brain_float_half
    )
    send_in = fill_slots(spread_in, positions, slot_count)
    send_grad = fill_slots(scaled, positions, slot_count)
    part_in, part_grad = (
        lax.all_to_all(send_in, "expert", split_axis=0, concat_axis=0, tiled=True),
        lax.all_to_all(send_grad, "expert", split_axis=0, concat_axis=0, tiled=True),
    )
    recv_in, recv_grad = (
        lax.all_gather(part_in, "tensor", axis=1, tiled=True),
        lax.all_gather(part_grad, "tensor", axis=1, tiled=True),
    )
    hidden_width = recv_in.shape[1]
    routed_input = recv_in.reshape(sources, local_experts, capacity, hidden_width)
    routed_gradient = recv_grad.reshape(sources, local_experts, capacity, hidden_width)
    slice_width = hidden_width // lax.axis_size("tensor")
    slice_start = lax.axis_index("tensor") * slice_width
    adapter_gate_term = jnp.einsum(
        "mbtk,bkz->mbtz", routed_input, gate_adapter_first, preferred_element_type=single_float
    ).astype(brain_float_half)
    adapter_up_term = jnp.einsum(
        "mbtk,bkz->mbtz", routed_input, up_adapter_first, preferred_element_type=single_float
    ).astype(brain_float_half)
    gate_activation = jnp.einsum(
        "secd,edf->secf", routed_input, gate_weight, preferred_element_type=single_float
    )
    gate_activation = gate_activation + adapter_scale * jnp.einsum(
        "imal,mlt->imat",
        adapter_gate_term,
        gate_adapter_second,
        preferred_element_type=single_float,
    )
    up_activation = jnp.einsum(
        "secd,edf->secf", routed_input, up_weight, preferred_element_type=single_float
    )
    up_activation = up_activation + adapter_scale * jnp.einsum(
        "imal,mlt->imat", adapter_up_term, up_adapter_second, preferred_element_type=single_float
    )
    sigma = jax.nn.sigmoid(gate_activation)
    active = gate_activation * sigma
    hidden_activation = (active * up_activation).astype(brain_float_half)
    down_part = jnp.einsum(
        "secf,efr->secr", hidden_activation, down_adapter_first, preferred_element_type=single_float
    )
    down_total = lax.psum(down_part.astype(jnp.bfloat16), "tensor").astype(jnp.float32)
    backward_adapter_term = jnp.einsum(
        "secd,erd->secr", routed_gradient, down_adapter_second, preferred_element_type=single_float
    ).astype(brain_float_half)
    hidden_gradient = jnp.einsum(
        "secd,efd->secf", routed_gradient, down_weight, preferred_element_type=single_float
    )
    hidden_gradient = hidden_gradient + adapter_scale * jnp.einsum(
        "oamh,ath->oamt",
        backward_adapter_term,
        down_adapter_first,
        preferred_element_type=single_float,
    )
    gate_gradient = (
        hidden_gradient * up_activation * sigma * (1.0 + gate_activation * (1.0 - sigma))
    ).astype(brain_float_half)
    upward_gradient = (hidden_gradient * active).astype(brain_float_half)
    gate_part = jnp.einsum(
        "secf,erf->secr", gate_gradient, gate_adapter_second, preferred_element_type=single_float
    )
    up_part = jnp.einsum(
        "secf,erf->secr", upward_gradient, up_adapter_second, preferred_element_type=single_float
    )
    joined_weight = jnp.concatenate(
        (gate_weight, up_weight, gate_adapter_first, up_adapter_first), axis=2
    )
    joined_grad = jnp.concatenate(
        (
            gate_gradient,
            upward_gradient,
            gate_part.astype(brain_float_half) * adapter_scale,
            up_part.astype(brain_float_half) * adapter_scale,
        ),
        axis=3,
    )
    input_portion = (
        jnp.einsum(
            "secf,edf->secd", joined_grad, joined_weight, preferred_element_type=single_float
        )
        .astype(brain_float_half)
        .reshape(slot_count, hidden_width)
    )
    gate_total, up_total = (
        lax.psum(gate_part.astype(jnp.bfloat16), "tensor").astype(jnp.float32),
        lax.psum(up_part.astype(jnp.bfloat16), "tensor").astype(jnp.float32),
    )
    in_slice = lax.dynamic_slice_in_dim(routed_input, slice_start, slice_width, 3)
    grad_slice = lax.dynamic_slice_in_dim(routed_gradient, slice_start, slice_width, 3)
    gate_first_gradient = adapter_scale * jnp.einsum(
        "secd,secr->edr",
        in_slice,
        gate_total.astype(brain_float_half),
        preferred_element_type=single_float,
    )
    up_first_gradient = adapter_scale * jnp.einsum(
        "secd,secr->edr",
        in_slice,
        up_total.astype(brain_float_half),
        preferred_element_type=single_float,
    )
    gate_second_gradient = adapter_scale * jnp.einsum(
        "zdbq,zdbx->dqx", adapter_gate_term, gate_gradient, preferred_element_type=single_float
    )
    up_second_gradient = adapter_scale * jnp.einsum(
        "zdbq,zdbx->dqx", adapter_up_term, upward_gradient, preferred_element_type=single_float
    )
    down_first_gradient = adapter_scale * jnp.einsum(
        "qoax,qoap->oxp",
        hidden_activation,
        backward_adapter_term,
        preferred_element_type=single_float,
    )
    down_second_gradient = adapter_scale * jnp.einsum(
        "secr,secd->erd",
        down_total.astype(brain_float_half),
        grad_slice,
        preferred_element_type=single_float,
    )
    reduced = lax.psum_scatter(
        input_portion.astype(single_float).astype(jnp.bfloat16),
        "tensor",
        scatter_dimension=1,
        tiled=True,
    ).astype(jnp.float32)
    returned = lax.all_to_all(
        reduced.astype(jnp.bfloat16), "expert", split_axis=0, concat_axis=0, tiled=True
    ).astype(reduced.dtype)
    grad_tokens = jnp.sum(returned[positions], axis=1).astype(brain_float_half)
    return (
        grad_tokens,
        gate_first_gradient,
        gate_second_gradient,
        up_first_gradient,
        up_second_gradient,
        down_first_gradient,
        down_second_gradient,
    )


def block_diagonal(blocks):
    count = len(blocks)
    rows = []
    for i, block in enumerate(blocks):
        rows.append(
            jnp.concatenate(
                [block if i == j else jnp.zeros_like(blocks[j]) for j in range(count)], axis=1
            )
        )
    return jnp.concatenate(rows, axis=0)


def diagonal_blocks(matrix, count):
    height, width = matrix.shape[0] // count, matrix.shape[1] // count
    return jnp.stack(
        [matrix[i * height : (i + 1) * height, i * width : (i + 1) * width] for i in range(count)]
    )


def widen(columns, width):
    rows, count = columns.shape
    return jnp.concatenate(
        [jnp.broadcast_to(columns[:, i : i + 1], (rows, width)) for i in range(count)], axis=1
    )


def dot(a, b):
    return lax.dot_general(a, b, (((1,), (0,)), ((), ())), preferred_element_type=jnp.float32)


def dot_t(a, b):
    return lax.dot_general(a, b, (((1,), (1,)), ((), ())), preferred_element_type=jnp.float32)


def t_dot(a, b):
    return lax.dot_general(a, b, (((0,), (0,)), ((), ())), preferred_element_type=jnp.float32)


def swap_near(value):
    count = lax.axis_size("tensor")
    return lax.ppermute(value, "tensor", [(i, i ^ 1) for i in range(count)])


def swap_far(value):
    count = lax.axis_size("tensor")
    return lax.ppermute(value, "tensor", [(i, (i + count // 2) % count) for i in range(count)])


def total_over_tensor(part):
    near = part.astype(jnp.bfloat16)
    pair = (near.astype(jnp.float32) + swap_near(near).astype(jnp.float32)).astype(jnp.bfloat16)
    return (pair.astype(jnp.float32) + swap_far(pair).astype(jnp.float32)).astype(jnp.bfloat16)


def gather_kernel(
    count,
    tokens_ref,
    grad_ref,
    chosen_ref,
    mine_ref,
    theirs_ref,
    chosen_all_ref,
    local_sem,
    far_send,
    far_recv,
    ring_send,
    ring_recv,
    near_send,
    near_recv,
    small_send,
    small_recv,
):
    me = lax.axis_index("expert")
    place = lax.axis_index("tensor")
    far, near = place // 2, place % 2
    rows, width = tokens_ref.shape
    depth = count // 2
    side = me % 2
    position = (1 - side) * (me // 2) + side * (count - 1 - me // 2)

    def expert_at(ring_place):
        ring_place = (ring_place + 2 * count) % count
        second = ring_place // depth
        return (1 - second) * 2 * ring_place + second * (2 * (count - 1 - ring_place) + 1)

    far_device = {"tensor": (1 - far) * 2 + near}
    near_device = {"tensor": far * 2 + 1 - near}
    barrier = pltpu.get_barrier_semaphore()
    pl.semaphore_signal(
        barrier, inc=1, device_id=far_device, device_id_type=pl.DeviceIdType.MESH
    )
    pl.semaphore_signal(
        barrier, inc=1, device_id=near_device, device_id_type=pl.DeviceIdType.MESH
    )
    for i in range(1, count):
        pl.semaphore_signal(
            barrier,
            inc=1,
            device_id={"expert": (me + i) % count},
            device_id_type=pl.DeviceIdType.MESH,
        )
    pl.semaphore_wait(barrier, count + 1)

    def remote(src, dst, send, recv, device):
        return pltpu.make_async_remote_copy(
            src_ref=src,
            dst_ref=dst,
            send_sem=send,
            recv_sem=recv,
            device_id=device,
            device_id_type=pl.DeviceIdType.MESH,
        )

    def columns(array, owner):
        return pl.ds(pl.multiple_of((2 * array + owner) * width, 128), width)

    sends, arrivals = [], []
    sources = (tokens_ref, grad_ref)
    for i, source in enumerate(sources):
        copy = remote(
            source,
            mine_ref.at[me, :, columns(i, far)],
            far_send.at[i],
            far_recv.at[i],
            far_device,
        )
        copy.start()
        sends.append(copy)
    own = [
        pltpu.make_async_copy(source, mine_ref.at[me, :, columns(i, far)], local_sem.at[i])
        for i, source in enumerate(sources)
    ]
    own.append(pltpu.make_async_copy(chosen_ref, chosen_all_ref.at[me], local_sem.at[2]))
    for copy in own:
        copy.start()
    for i in range(1, count):
        copy = remote(
            chosen_ref,
            chosen_all_ref.at[me],
            small_send.at[i - 1],
            small_recv.at[i - 1],
            {"expert": (me + i) % count},
        )
        copy.start()
        sends.append(copy)
        arrivals.append(
            remote(
                chosen_ref,
                chosen_all_ref.at[(me + count - i) % count],
                small_send.at[i - 1],
                small_recv.at[i - 1],
                {"expert": (me + i) % count},
            )
        )
    for copy in own:
        copy.wait()
    for i, source in enumerate(sources):
        remote(
            source,
            mine_ref.at[me, :, columns(i, 1 - far)],
            far_send.at[i],
            far_recv.at[i],
            far_device,
        ).wait_recv()

    def share(block, slot):
        copy = remote(
            mine_ref.at[block],
            theirs_ref.at[block],
            near_send.at[slot],
            near_recv.at[slot],
            near_device,
        )
        copy.start()
        sends.append(copy)
        arrivals.append(copy)

    def part(step, way, block):
        if step < depth - 1:
            return mine_ref.at[block]
        return mine_ref.at[block, pl.ds(way * (rows // 2), rows // 2)]

    for step in range(depth):
        for way, sign in ((0, 1), (1, -1)):
            block = expert_at(position - sign * step)
            piece = part(step, way, block)
            copy = remote(
                piece,
                piece,
                ring_send.at[way, step],
                ring_recv.at[way, step],
                {"expert": expert_at(position + sign)},
            )
            copy.start()
            sends.append(copy)
        if step == 0:
            share(me, 0)
        else:
            for way, sign in ((0, 1), (1, -1)):
                share(expert_at(position - sign * step), 2 * step - 1 + way)
        for way, sign in ((0, 1), (1, -1)):
            block = expert_at(position - sign * (step + 1))
            piece = part(step, way, block)
            remote(
                piece,
                piece,
                ring_send.at[way, step],
                ring_recv.at[way, step],
                {"expert": expert_at(position + sign)},
            ).wait_recv()
    share(expert_at(position + depth), count - 1)
    for copy in arrivals:
        copy.wait_recv()
    for copy in sends:
        copy.wait_send()


def gather_all(tokens, grad_out, chosen):
    count = lax.axis_size("expert")
    rows, width = tokens.shape
    block = jax.ShapeDtypeStruct((count, rows, 4 * width), tokens.dtype)
    dma = pltpu.SemaphoreType.DMA
    return pl.pallas_call(
        functools.partial(gather_kernel, count),
        out_shape=(block, block, jax.ShapeDtypeStruct((count,) + chosen.shape, chosen.dtype)),
        in_specs=[pl.BlockSpec(memory_space=pltpu.VMEM)] * 3,
        out_specs=[pl.BlockSpec(memory_space=pltpu.VMEM)] * 3,
        scratch_shapes=[
            dma((3,)),
            dma((2,)),
            dma((2,)),
            dma((2, count // 2)),
            dma((2, count // 2)),
            dma((count,)),
            dma((count,)),
            dma((count - 1,)),
            dma((count - 1,)),
        ],
        compiler_params=pltpu.CompilerParams(
            collective_id=0, has_side_effects=True, vmem_limit_bytes=32 * 2**20
        ),
    )(tokens, grad_out, chosen)


def dense_plan(
    tokens,
    grad_out,
    route_weights,
    expert_ids,
    gate_weight,
    up_weight,
    down_weight,
    gate_adapter_first,
    gate_adapter_second,
    up_adapter_first,
    up_adapter_second,
    down_adapter_first,
    down_adapter_second,
):
    half = jnp.bfloat16
    single = jnp.float32
    tok_rows, width = tokens.shape
    local_experts, hidden_width, units = gate_weight.shape
    rank = gate_adapter_first.shape[2]
    experts_all = local_experts * lax.axis_size("expert")
    span = local_experts * units
    ranks = local_experts * rank
    place = lax.axis_index("tensor")
    far, near = place // 2, place % 2

    numbers = lax.broadcasted_iota(jnp.int32, (1, 1, experts_all), 2)
    chosen = jnp.sum(
        jnp.where(expert_ids[:, :, None] == numbers, route_weights[:, :, None], 0.0), axis=1
    )
    mine, theirs, chosen_all = gather_all(tokens, grad_out, chosen.T)
    mine = mine.reshape(-1, 4 * width)
    theirs = theirs.reshape(-1, 4 * width)
    chosen_all = lax.dynamic_slice_in_dim(
        chosen_all, lax.axis_index("expert") * local_experts, local_experts, 1
    )
    factor = chosen_all.transpose(0, 2, 1).reshape(-1, local_experts)
    experts = range(local_experts)

    def pick(weight, core, axis):
        pieces = [
            lax.dynamic_slice_in_dim(weight, (2 * i + core) * width, width, axis) for i in range(2)
        ]
        return jnp.concatenate(pieces, axis=axis)

    def joined_rows(core):
        arrays = (gate_weight, up_weight, gate_adapter_first, up_adapter_first)
        return jnp.concatenate([pick(w[e], core, 0) for w in arrays for e in experts], axis=1)

    def back_columns(core):
        arrays = (down_weight, down_adapter_second)
        return jnp.concatenate([pick(w[e], core, 1) for w in arrays for e in experts], axis=0)

    joined_keep, joined_give = joined_rows(near), joined_rows(1 - near)
    back_keep, back_give = back_columns(near), back_columns(1 - near)
    gate_second = block_diagonal([gate_adapter_second[e] for e in experts])
    up_second = block_diagonal([up_adapter_second[e] for e in experts])
    down_first = block_diagonal([down_adapter_first[e] for e in experts])
    factor_units = widen(factor, units)
    factor_ranks = widen(factor, rank)

    forward = dot(mine[:, : 2 * width], joined_keep) + dot(theirs[:, : 2 * width], joined_give)
    lora_gate = forward[:, 2 * span : 2 * span + ranks].astype(half)
    lora_up = forward[:, 2 * span + ranks :].astype(half)
    gate = forward[:, :span] + adapter_scale * dot(lora_gate, gate_second)
    up = forward[:, span : 2 * span] + adapter_scale * dot(lora_up, up_second)
    sigma = jax.nn.sigmoid(gate)
    active = gate * sigma
    hidden = (active * up).astype(half)
    down_total = total_over_tensor(dot(hidden, down_first))

    backward = dot_t(mine[:, 2 * width :], back_keep) + dot_t(theirs[:, 2 * width :], back_give)
    back_lora = (factor_ranks * backward[:, span:]).astype(half)
    grad_hidden = factor_units * backward[:, :span] + adapter_scale * dot_t(back_lora, down_first)
    grad_gate = (grad_hidden * up * sigma * (1.0 + gate * (1.0 - sigma))).astype(half)
    grad_up = (grad_hidden * active).astype(half)
    parts = jnp.concatenate((dot_t(grad_gate, gate_second), dot_t(grad_up, up_second)), axis=1)
    parts = parts.astype(half)
    joined_grad = jnp.concatenate((grad_gate, grad_up, parts * adapter_scale), axis=1)
    give = swap_near(dot_t(joined_grad, joined_give).astype(half))
    keep = dot_t(joined_grad, joined_keep).astype(half)
    pair = (keep.astype(single) + give.astype(single)).astype(half)
    summed = lax.psum_scatter(pair, "expert", scatter_dimension=0, tiled=True)
    summed_keep = lax.dynamic_slice_in_dim(summed, far * width, width, 1)
    summed_give = lax.dynamic_slice_in_dim(summed, (1 - far) * width, width, 1)
    grad_tokens = (summed_keep.astype(single) + swap_far(summed_give).astype(single)).astype(half)

    parts_total = total_over_tensor(parts)
    in_slice = lax.dynamic_slice_in_dim(mine, far * width, width, 1)
    grad_slice = lax.dynamic_slice_in_dim(mine, (2 + far) * width, width, 1)
    first = adapter_scale * t_dot(in_slice, parts_total)
    first = first.reshape(width, 2, local_experts, rank).transpose(1, 2, 0, 3)
    weighted = (factor_ranks * down_total.astype(single)).astype(half)
    down_second_gradient = adapter_scale * t_dot(weighted, grad_slice)
    return (
        grad_tokens,
        first[0],
        diagonal_blocks(adapter_scale * t_dot(lora_gate, grad_gate), local_experts),
        first[1],
        diagonal_blocks(adapter_scale * t_dot(lora_up, grad_up), local_experts),
        diagonal_blocks(adapter_scale * t_dot(hidden, back_lora), local_experts),
        down_second_gradient.reshape(local_experts, rank, width),
    )


def local(*arrays):
    tok_rows, top_count = arrays[3].shape
    local_experts = arrays[4].shape[0]
    capacity = 3 * tok_rows * top_count // (2 * local_experts * lax.axis_size("expert"))
    if local_experts * capacity >= tok_rows and lax.axis_size("tensor") == 2 * 2:
        return dense_plan(*arrays)
    return routed_plan(*arrays)


def solution(mesh):
    return jax.shard_map(
        local,
        mesh=mesh,
        in_specs=(
            P("expert", "tensor"),
            P("expert", "tensor"),
            P("expert", None),
            P("expert", None),
            P("expert", None, "tensor"),
            P("expert", None, "tensor"),
            P("expert", "tensor", None),
            P("expert", None, None),
            P("expert", None, "tensor"),
            P("expert", None, None),
            P("expert", None, "tensor"),
            P("expert", "tensor", None),
            P("expert", None, None),
        ),
        out_specs=(
            P("expert", "tensor"),
            P("expert", "tensor", None),
            P("expert", None, "tensor"),
            P("expert", "tensor", None),
            P("expert", None, "tensor"),
            P("expert", "tensor", None),
            P("expert", None, "tensor"),
        ),
        check_vma=False,
    )
```
